32 devices in a mesh: scale: 2 (over y), lat: 16 (over z, x, core).
Axes of the slice: x: 2, y: 2, z: 4, core: 2. Of those that a mesh axis runs over, the one named last changes fastest.
Arguments:
- fine_state: float32 [16, 2, 1280, 1280], P(None, None, ('scale', 'lat')), may hold values from -6 to 6
- fine_noise: bfloat16 [16, 2, 1280, 1280], P(None, None, ('scale', 'lat')), may hold values from -6 to 6
- medium_state: float32 [16, 2, 640, 640], P(None, None, ('scale', 'lat')), may hold values from -6 to 6
- medium_noise: bfloat16 [16, 2, 640, 640], P(None, None, ('scale', 'lat')), may hold values from -6 to 6
- coarse_state: float32 [16, 2, 160, 160], P('lat'), may hold values from -6 to 6
- coarse_noise: bfloat16 [16, 2, 160, 160], P('lat'), may hold values from -6 to 6
- decay: float32 [3], replicated, may hold values from 0.5 to 0.95
- amplitude: float32 [3], replicated, may hold values from 0.3 to 1
- fine_basis: bfloat16 [1280, 32, 1280], P(('scale', 'lat')), may hold values from -0.0017089844 to 0.0017089844
- medium_basis: bfloat16 [640, 32, 640], P(('scale', 'lat')), may hold values from -0.0034179688 to 0.0034179688
- coarse_basis: bfloat16 [32, 160, 160], P(('scale', 'lat')), may hold values from -0.013671875 to 0.013671875
Outputs:
- fine_next: float32 [16, 2, 1280, 1280], P(None, None, ('scale', 'lat'))
- medium_next: float32 [16, 2, 640, 640], P(None, None, ('scale', 'lat'))
- coarse_next: float32 [16, 2, 160, 160], P('lat')
- pattern: float32 [16, 32, 2560], P(None, ('scale', 'lat'))
The draws below stay inside these ranges and needn't reach their ends.
All inputs are finite; a program needn't handle non-finite values.
Results may differ from the reference program's by a relative error of at most 0.005.
Values may be sent and summed in bfloat16 or wider, within the bound.
A program may use at most 128 MiB of HBM per device.

```python
import math
import jax
import jax.numpy as jnp
from jax import lax

MF = 1280
MM = 640
MC = 160
NLON = 2560
MEMBERS = 16
NROWS = 32


def shard_levels(own_key, dims, shards, smallest, largest):
    factor_of, own = 1.0, jax.random.fold_in(own_key, 6)
    for position, shards_of in shards:
        draws = jnp.exp(jax.random.uniform(jax.random.fold_in(own, position), (shards_of,), jnp.float32, smallest / len(shards), largest / len(shards)))
        factor_of = factor_of * jnp.repeat(draws, dims[position] // shards_of).reshape([-1 if axis == position else 1 for axis in range(len(dims))])
    return factor_of


def gaussian(own_key, dims, width, bound, pieces=(), held_as=jnp.bfloat16):
    factor_of = shard_levels(own_key, dims, pieces, -0.22, 0.18) if pieces else 1.0
    drawn = jax.random.normal(own_key, dims, jnp.float32) * width * factor_of
    return jnp.minimum(jnp.maximum(drawn, -bound), bound).astype(held_as)


def setup_inputs(seed: int = 0) -> dict:
    splits = jax.random.split(jax.random.key(seed), 12)
    fine_state = gaussian(splits[0], (MEMBERS, 2, MF, MF), 1.0, 6.0, ((2, 32),), jnp.float32)
    fine_noise = gaussian(splits[1], (MEMBERS, 2, MF, MF), 1.0, 6.0, ((2, 32),))
    medium_state = gaussian(splits[2], (MEMBERS, 2, MM, MM), 1.0, 6.0, ((2, 32),), jnp.float32)
    medium_noise = gaussian(splits[3], (MEMBERS, 2, MM, MM), 1.0, 6.0, ((2, 32),))
    coarse_state = gaussian(splits[4], (MEMBERS, 2, MC, MC), 1.0, 6.0, ((0, 16),), jnp.float32)
    coarse_noise = gaussian(splits[5], (MEMBERS, 2, MC, MC), 1.0, 6.0, ((0, 16),))
    decay = jnp.clip(jax.random.uniform(splits[6], (3,), jnp.float32, 0.5, 0.95), 0.5, 0.95)
    amplitude = jnp.clip(jax.random.uniform(splits[7], (3,), jnp.float32, 0.3, 1.0), 0.3, 1.0)
    fine_basis = gaussian(splits[8], (MF, NROWS, MF), (8 * MF * MF) ** -0.5, 0.0017089844, ((0, 32),))
    medium_basis = gaussian(splits[9], (MM, NROWS, MM), (8 * MM * MM) ** -0.5, 0.0034179688, ((0, 32),))
    coarse_basis = gaussian(splits[10], (NROWS, MC, MC), (8 * MC * MC) ** -0.5, 0.013671875, ((0, 32),))
    return {"fine_state": fine_state, "fine_noise": fine_noise, "medium_state": medium_state, "medium_noise": medium_noise, "coarse_state": coarse_state, "coarse_noise": coarse_noise, "decay": decay, "amplitude": amplitude, "fine_basis": fine_basis, "medium_basis": medium_basis, "coarse_basis": coarse_basis}


def advance(state, noise, decay_rate, amp_rate):
    slots = state.shape[3]
    mode_ids = jnp.arange(state.shape[2], dtype=jnp.int32)
    degree_ids = jnp.arange(slots, dtype=jnp.int32)
    inside = (mode_ids[:, None] + degree_ids[None, :]) < slots
    updated = decay_rate * state + amp_rate * noise.astype(jnp.float32)
    return jnp.where(inside, updated, jnp.zeros_like(updated))


def legendre_by_modes(half, basis):
    members, parts, modes, slots = half.shape
    nrow = basis.shape[1]
    blocks = modes // 32
    coef_blocks = jnp.moveaxis(half.reshape(members, parts, blocks, 32, slots), 2, 0)
    basis_blocks = basis.reshape(blocks, 32, nrow, slots)

    def one_block(pair):
        return jnp.einsum("ecmk,mrk->ecmr", pair[0].astype(jnp.float32), pair[1].astype(jnp.float32))

    result = lax.map(one_block, (coef_blocks, basis_blocks))
    return jnp.moveaxis(result, 0, 2).reshape(members, parts, modes, nrow)


def grid_table(modes):
    mode_ids = jnp.arange(modes, dtype=jnp.int32)
    lon_ids = jnp.arange(NLON, dtype=jnp.int32)
    angles = ((mode_ids[:, None] * lon_ids[None, :]) % NLON).astype(jnp.float32) * (2.0 * math.pi / NLON)
    weights = jnp.where(mode_ids == 0, 1.0, 2.0).astype(jnp.float32)[:, None]
    return jnp.stack([weights * jnp.cos(angles), -weights * jnp.sin(angles)]).astype(jnp.bfloat16)


def synthesis(fourier):
    table = grid_table(fourier.shape[2])
    return jnp.einsum("ecmr,cml->erl", fourier.astype(jnp.float32), table.astype(jnp.float32))


def reference(fine_state, fine_noise, medium_state, medium_noise, coarse_state, coarse_noise, decay, amplitude, fine_basis, medium_basis, coarse_basis):
    fine_next = advance(fine_state, fine_noise, decay[0], amplitude[0])
    medium_next = advance(medium_state, medium_noise, decay[1], amplitude[1])
    coarse_next = advance(coarse_state, coarse_noise, decay[2], amplitude[2])
    fine_fourier = legendre_by_modes(fine_next.astype(jnp.bfloat16), fine_basis).astype(jnp.bfloat16)
    medium_fourier = legendre_by_modes(medium_next.astype(jnp.bfloat16), medium_basis).astype(jnp.bfloat16)
    coarse_fourier = jnp.einsum("ecmk,rmk->ecmr", coarse_next.astype(jnp.bfloat16).astype(jnp.float32), coarse_basis.astype(jnp.float32)).astype(jnp.bfloat16)
    total = synthesis(fine_fourier) + synthesis(medium_fourier) + synthesis(coarse_fourier)
    pattern = jnp.tanh(total).astype(jnp.float32)
    return fine_next, medium_next, coarse_next, pattern
```

```python
import math

import jax
import jax.numpy as jnp
from jax import lax
from jax.sharding import PartitionSpec as P

NLON = 2560
LANES = 128
FOLD = NLON // LANES


def advance(state, noise, decay_rate, amp_rate, offset):
    slots = state.shape[3]
    mode_ids = offset + jnp.arange(state.shape[2], dtype=jnp.int32)
    degree_ids = jnp.arange(slots, dtype=jnp.int32)
    inside = mode_ids[:, None] + degree_ids[None, :] < slots
    updated = decay_rate * state + amp_rate * noise.astype(jnp.float32)
    return jnp.where(inside, updated, jnp.zeros_like(updated))


def angle_tables(high):
    lon = jnp.arange(LANES, dtype=jnp.int32)
    hi = (jnp.arange(high, dtype=jnp.int32)[:, None] * lon[None, :] % LANES).astype(jnp.float32)
    lo = (jnp.arange(FOLD, dtype=jnp.int32)[:, None] * lon[None, :]).astype(jnp.float32)
    hi, lo = lax.optimization_barrier(
        (
            jnp.stack([jnp.cos(hi * (2 * math.pi / LANES)), jnp.sin(hi * (2 * math.pi / LANES))]),
            jnp.stack([jnp.cos(lo * (2 * math.pi / NLON)), jnp.sin(lo * (2 * math.pi / NLON))]),
        )
    )
    ch, sh = hi[0][:, None, :], hi[1][:, None, :]
    cl, sl = lo[0][None], lo[1][None]
    first = (jnp.arange(high) == 0)[:, None, None] & (jnp.arange(FOLD) == 0)[None, :, None]
    weight = jnp.where(first, 1.0, 2.0).astype(jnp.float32)
    cos, sin = weight * (ch * cl - sh * sl), weight * (sh * cl + ch * sl)
    table = jnp.stack(
        [jnp.concatenate([cos, sin], axis=-1), jnp.concatenate([-sin, cos], axis=-1)]
    )
    return table.astype(jnp.bfloat16)


def body(
    fine_state,
    fine_noise,
    medium_state,
    medium_noise,
    coarse_state,
    coarse_noise,
    decay,
    amplitude,
    fine_basis,
    medium_basis,
    coarse_basis,
):
    place = lax.axis_index(("scale", "lat"))
    fine_next = advance(fine_state, fine_noise, decay[0], amplitude[0], place * fine_state.shape[2])
    medium_next = advance(
        medium_state, medium_noise, decay[1], amplitude[1], place * medium_state.shape[2]
    )
    coarse_next = advance(coarse_state, coarse_noise, decay[2], amplitude[2], 0)
    devices = lax.axis_size("scale") * lax.axis_size("lat")
    part_modes = -(-coarse_next.shape[2] // devices)
    modes = coarse_next.shape[2]
    grow = ((0, 0), (0, 0), (0, part_modes * devices - modes), (0, 0))
    held, own, slots = coarse_next.shape[0], coarse_basis.shape[0], coarse_next.shape[3]
    mine = jnp.concatenate(
        [coarse_next.astype(jnp.bfloat16).reshape(held * 2, modes, slots), coarse_basis], axis=0
    )
    mine = jnp.pad(mine, grow[1:]).reshape(-1, devices, part_modes * slots).swapaxes(0, 1)
    mixed = lax.all_to_all(mine, ("scale", "lat"), split_axis=0, concat_axis=0, tiled=True)
    mixed = mixed.reshape(devices, 2 * held + own, part_modes, slots)
    lat = lax.axis_size("lat")
    coarse_half = mixed[:lat, : 2 * held].reshape(lat * held, 2, part_modes, slots)
    coarse_rows = mixed[:, 2 * held :].reshape(devices * own, part_modes, slots)
    fourier = []
    for half, basis, form in (
        (fine_next.astype(jnp.bfloat16), fine_basis, "ecmk,mrk->rcme"),
        (medium_next.astype(jnp.bfloat16), medium_basis, "ecmk,mrk->rcme"),
        (coarse_half, coarse_rows, "ecmk,rmk->rcme"),
    ):
        fourier.append(
            jnp.einsum(form, half, basis, preferred_element_type=jnp.float32).astype(jnp.bfloat16)
        )
    members = coarse_half.shape[0]
    mf, mm = fine_state.shape[2], medium_state.shape[2]
    rows = fine_basis.shape[1]
    both = jnp.concatenate(fourier, axis=2).reshape(rows, 2, (mf + mm + part_modes) * members)
    got = lax.all_to_all(both, ("scale", "lat"), split_axis=0, concat_axis=0, tiled=True)
    got = got.reshape(devices, own, 2, mf + mm + part_modes, members)
    got = got.transpose(1, 2, 0, 3, 4)

    def fold(x):
        return x.reshape(own, 2, -1, FOLD, members)

    fine = fold(got[:, :, :, :mf])
    medium = fold(got[:, :, :, mf : mf + mm])
    coarse = got[:, :, :, mf + mm :].reshape(own, 2, devices * part_modes, members)
    coarse = fold(coarse[:, :, :modes])
    table = angle_tables(fine.shape[2])
    stacked = jnp.concatenate([fine, medium, coarse], axis=2)
    stacked_table = jnp.concatenate(
        [table, table[:, : medium.shape[2]], table[:, : coarse.shape[2]]], axis=1
    )
    part = jnp.einsum(
        "rchqe,chqx->reqx", stacked, stacked_table, preferred_element_type=jnp.float32
    ).reshape(own, members, FOLD, 2, LANES)
    angle = (
        (jnp.arange(FOLD)[:, None] * jnp.arange(FOLD)[None, :] % FOLD).astype(jnp.float32)
        * (2 * math.pi / FOLD)
    )
    turn = jnp.stack([jnp.cos(angle), -jnp.sin(angle)], axis=1)
    total = jnp.einsum("reqxl,qxh->erhl", part, turn, precision=lax.Precision.HIGHEST)
    pattern = jnp.tanh(total.reshape(members, own, NLON))
    return (fine_next, medium_next, coarse_next, pattern)


def solution(mesh):
    return jax.shard_map(
        body,
        mesh=mesh,
        in_specs=(
            P(None, None, ("scale", "lat"), None),
            P(None, None, ("scale", "lat"), None),
            P(None, None, ("scale", "lat"), None),
            P(None, None, ("scale", "lat"), None),
            P("lat", None, None, None),
            P("lat", None, None, None),
            P(),
            P(),
            P(("scale", "lat"), None, None),
            P(("scale", "lat"), None, None),
            P(("scale", "lat"), None, None),
        ),
        out_specs=(
            P(None, None, ("scale", "lat"), None),
            P(None, None, ("scale", "lat"), None),
            P("lat", None, None, None),
            P(None, ("scale", "lat"), None),
        ),
        check_vma=False,
    )
```

```python
import functools
import math

import jax
import jax.numpy as jnp
from jax import lax
from jax.experimental import pallas as pl
from jax.experimental.pallas import tpu as pltpu
from jax.sharding import PartitionSpec as P

NLON = 2560
LANES = 128
FOLD = NLON // LANES


def advance(state, noise, decay_rate, amp_rate, offset):
    slots = state.shape[3]
    mode_ids = offset + jnp.arange(state.shape[2], dtype=jnp.int32)
    degree_ids = jnp.arange(slots, dtype=jnp.int32)
    inside = mode_ids[:, None] + degree_ids[None, :] < slots
    updated = decay_rate * state + amp_rate * noise.astype(jnp.float32)
    return jnp.where(inside, updated, jnp.zeros_like(updated))


def phase_rows(block, devices):
    return max((p * block % FOLD + block - 1) // FOLD + 1 for p in range(devices))


def phase_blocks(fourier, place, devices, modes=None):
    rows, parts, block, members = fourier.shape
    high = phase_rows(block, devices)
    if block % FOLD:
        start = (place * block % FOLD).astype(jnp.int32)
        room = jnp.zeros((rows, parts, high * FOLD, members), fourier.dtype)
        zero = jnp.zeros((), jnp.int32)
        fourier = lax.dynamic_update_slice(room, fourier, (zero, zero, start, zero))
    return fourier.reshape(rows, parts * high, FOLD * members)


def base_phases(blocks, devices, width):
    source = jnp.arange(devices, dtype=jnp.int32)[:, None]
    cols, parts = [], []
    for block in blocks:
        for part in range(2):
            for j in range(phase_rows(block, devices)):
                cols.append(source * block // FOLD + j)
                parts.append(part)
    while len(cols) < width:
        cols.append(source * 0)
        parts.append(0)
    high = jnp.concatenate(cols, axis=1).reshape(-1, 1)
    part = jnp.tile(jnp.array(parts, jnp.int32), devices)[:, None]
    lon = jnp.arange(LANES, dtype=jnp.int32)[None, :]
    turns = (high * lon + part * (LANES // 4)) % LANES
    angle = turns.astype(jnp.float32) * (2.0 * math.pi / LANES)
    first = jnp.where(high == 0, 0.5, 1.0).astype(jnp.float32) * jnp.ones_like(angle)
    low = (jnp.arange(FOLD, dtype=jnp.int32)[:, None] * lon).astype(jnp.float32) * (
        2.0 * math.pi / NLON
    )
    return (
        jnp.stack([2.0 * jnp.cos(angle), 2.0 * jnp.sin(angle), first]),
        jnp.stack([jnp.cos(low), jnp.sin(low)]),
    )


def longitude_kernel(members, got_ref, base_ref, low_ref, out_ref):
    own = got_ref.shape[1]
    for i in range(own):
        spread = got_ref[:, i].astype(jnp.float32)
        spread = spread.reshape(spread.shape[0] * spread.shape[1], spread.shape[2])
        lanes = -spread.shape[1] % LANES
        if lanes:
            spread = jnp.concatenate(
                [spread, jnp.zeros((spread.shape[0], lanes), jnp.float32)], axis=1
            )
        turned = spread.T.astype(jnp.bfloat16)
        totals = [None] * FOLD
        for q in range(FOLD):
            re, im = base_ref[0], base_ref[1]
            if q == 0:
                re, im = re * base_ref[2], im * base_ref[2]
            cl, sl = low_ref[0, q : q + 1], low_ref[1, q : q + 1]
            table = jnp.concatenate([re * cl - im * sl, im * cl + re * sl], axis=1)
            part = jnp.dot(
                turned[q * members : (q + 1) * members],
                table.astype(jnp.bfloat16),
                preferred_element_type=jnp.float32,
            )
            real, imag = part[:, :LANES], part[:, LANES:]
            for h in range(FOLD):
                turn = 2.0 * math.pi * (q * h % FOLD) / FOLD
                term = math.cos(turn) * real - math.sin(turn) * imag
                totals[h] = term if q == 0 else totals[h] + term
        for h in range(FOLD):
            out_ref[:, i, h * LANES : (h + 1) * LANES] = jnp.tanh(totals[h])


def coarse_kernel(
    part_modes, decay_ref, amp_ref, state_ref, noise_ref, basis_ref, next_ref, mixed_ref
):
    held, parts, modes, slots = state_ref.shape
    mode_ids = lax.broadcasted_iota(jnp.int32, (modes, slots), 0)
    degree_ids = lax.broadcasted_iota(jnp.int32, (modes, slots), 1)
    inside = mode_ids + degree_ids < slots
    planes = []
    for e in range(held):
        for c in range(parts):
            new = decay_ref[2] * state_ref[e, c] + amp_ref[2] * noise_ref[e, c].astype(jnp.float32)
            new = jnp.where(inside, new, 0.0)
            next_ref[e, c] = new
            planes.append(new)
    for r in range(basis_ref.shape[0]):
        planes.append(basis_ref[r].astype(jnp.float32))
    empty = jnp.zeros((part_modes, slots), jnp.float32)
    for d in range(mixed_ref.shape[0]):
        pieces = []
        for plane in planes:
            piece = plane[d * part_modes : min((d + 1) * part_modes, modes)]
            missing = part_modes - piece.shape[0]
            if missing == part_modes:
                piece = empty
            elif missing:
                piece = jnp.concatenate([piece, empty[:missing]], axis=0)
            pieces.append(piece)
        mixed_ref[d] = jnp.concatenate(pieces, axis=0).astype(jnp.bfloat16)


def body(
    fine_state,
    fine_noise,
    medium_state,
    medium_noise,
    coarse_state,
    coarse_noise,
    decay,
    amplitude,
    fine_basis,
    medium_basis,
    coarse_basis,
):
    devices = lax.axis_size("scale") * lax.axis_size("lat")
    lat = lax.axis_size("lat")
    held, _, modes, slots = coarse_state.shape
    own = coarse_basis.shape[0]
    part_modes = -(-modes // devices)
    vmem = pl.BlockSpec(memory_space=pltpu.VMEM)
    smem = pl.BlockSpec(memory_space=pltpu.SMEM)
    coarse_next, mixed = pl.pallas_call(
        functools.partial(coarse_kernel, part_modes),
        out_shape=(
            jax.ShapeDtypeStruct(coarse_state.shape, jnp.float32),
            jax.ShapeDtypeStruct((devices, (2 * held + own) * part_modes, slots), jnp.bfloat16),
        ),
        in_specs=[smem, smem, vmem, vmem, vmem],
        out_specs=(vmem, vmem),
    )(decay, amplitude, coarse_state, coarse_noise, coarse_basis)
    mixed = lax.all_to_all(mixed, ("scale", "lat"), split_axis=0, concat_axis=0, tiled=True)
    mixed = mixed.reshape(devices, 2 * held + own, part_modes, slots)
    coarse_half = mixed[:lat, : 2 * held].reshape(lat * held, 2, part_modes, slots)
    coarse_rows = mixed[:, 2 * held :].reshape(devices * own, part_modes, slots)
    place = lax.axis_index(("scale", "lat"))
    fine_next = advance(fine_state, fine_noise, decay[0], amplitude[0], place * fine_state.shape[2])
    medium_next = advance(
        medium_state, medium_noise, decay[1], amplitude[1], place * medium_state.shape[2]
    )
    fourier = []
    for half, basis, form in (
        (fine_next.astype(jnp.bfloat16), fine_basis, "ecmk,mrk->rcme"),
        (medium_next.astype(jnp.bfloat16), medium_basis, "ecmk,mrk->rcme"),
        (coarse_half, coarse_rows, "ecmk,rmk->rcme"),
    ):
        fourier.append(
            jnp.einsum(form, half, basis, preferred_element_type=jnp.float32).astype(jnp.bfloat16)
        )
    members = coarse_half.shape[0]
    blocks = [x.shape[2] for x in fourier]
    both = jnp.concatenate([phase_blocks(x, place, devices) for x in fourier], axis=1)
    width = -(-both.shape[1] // 8) * 8
    both = jnp.pad(both, ((0, 0), (0, width - both.shape[1]), (0, 0)))
    got = lax.all_to_all(both, ("scale", "lat"), split_axis=0, concat_axis=0, tiled=True)
    got = got.reshape(devices, own, width, FOLD * members)
    base, low = base_phases(blocks, devices, width)
    pattern = pl.pallas_call(
        functools.partial(longitude_kernel, members),
        out_shape=jax.ShapeDtypeStruct((members, own, NLON), jnp.float32),
        in_specs=[vmem, vmem, vmem],
        out_specs=vmem,
    )(got, base, low)
    return (fine_next, medium_next, coarse_next, pattern)


def solution(mesh):
    return jax.shard_map(
        body,
        mesh=mesh,
        in_specs=(
            P(None, None, ("scale", "lat"), None),
            P(None, None, ("scale", "lat"), None),
            P(None, None, ("scale", "lat"), None),
            P(None, None, ("scale", "lat"), None),
            P("lat", None, None, None),
            P("lat", None, None, None),
            P(),
            P(),
            P(("scale", "lat"), None, None),
            P(("scale", "lat"), None, None),
            P(("scale", "lat"), None, None),
        ),
        out_specs=(
            P(None, None, ("scale", "lat"), None),
            P(None, None, ("scale", "lat"), None),
            P("lat", None, None, None),
            P(None, ("scale", "lat"), None),
        ),
        check_vma=False,
    )
```

```python
import functools
import math

import jax
import jax.numpy as jnp
import numpy as np
from jax import lax
from jax.experimental import pallas as pl
from jax.experimental.pallas import tpu as pltpu
from jax.sharding import PartitionSpec as P

NLON = 2560
LANES = 128
FOLD = NLON // LANES


def advance(state, noise, decay_rate, amp_rate, offset):
    slots = state.shape[3]
    mode_ids = offset + jnp.arange(state.shape[2], dtype=jnp.int32)
    degree_ids = jnp.arange(slots, dtype=jnp.int32)
    inside = mode_ids[:, None] + degree_ids[None, :] < slots
    updated = decay_rate * state + amp_rate * noise.astype(jnp.float32)
    return jnp.where(inside, updated, jnp.zeros_like(updated))


def phase_rows(block, devices):
    return max((p * block % FOLD + block - 1) // FOLD + 1 for p in range(devices))


def phase_blocks(fourier, place, devices, modes=None):
    rows, parts, block, members = fourier.shape
    high = phase_rows(block, devices)
    if block % FOLD:
        start = (place * block % FOLD).astype(jnp.int32)
        room = jnp.zeros((rows, parts, high * FOLD, members), fourier.dtype)
        zero = jnp.zeros((), jnp.int32)
        fourier = lax.dynamic_update_slice(room, fourier, (zero, zero, start, zero))
    return fourier.reshape(rows, parts * high, FOLD * members)


def received_rows(blocks, devices, width):
    source = np.arange(devices, dtype=np.int32)
    cols, parts = [], []
    for block in blocks:
        for part in range(2):
            for j in range(phase_rows(block, devices)):
                cols.append(source * block // FOLD + j)
                parts.append(part)
    while len(cols) < width:
        cols.append(source * 0)
        parts.append(0)
    high = np.stack(cols, axis=1).reshape(-1, 1)
    part = np.tile(np.array(parts, np.int32), devices)[:, None]
    return np.concatenate([high, part], axis=1).astype(np.int32)


def table_kernel(rows_ref, table_ref):
    count = rows_ref.shape[0]
    high, part = rows_ref[:, 0:1], rows_ref[:, 1:2]
    lon = lax.broadcasted_iota(jnp.int32, (count, LANES), 1)
    turns = (high * lon + part * (LANES // 4)) % LANES
    angle = turns.astype(jnp.float32) * (2.0 * math.pi / LANES)
    re, im = 2.0 * jnp.cos(angle), 2.0 * jnp.sin(angle)
    first = jnp.where(high == 0, 0.5, 1.0).astype(jnp.float32)
    shape = (-(-FOLD // 8) * 8, LANES)
    low = lax.broadcasted_iota(jnp.int32, shape, 0) * lax.broadcasted_iota(jnp.int32, shape, 1)
    low = low.astype(jnp.float32) * (2.0 * math.pi / NLON)
    cos, sin = jnp.cos(low), jnp.sin(low)
    for q in range(FOLD):
        cl, sl = cos[q : q + 1], sin[q : q + 1]
        real, imag = re * cl - im * sl, im * cl + re * sl
        if q == 0:
            real, imag = real * first, imag * first
        table_ref[q, :, :LANES] = real.astype(jnp.bfloat16)
        table_ref[q, :, LANES:] = imag.astype(jnp.bfloat16)


def longitude_kernel(members, got_ref, table_ref, out_ref):
    own = got_ref.shape[1]
    for i in range(own):
        spread = got_ref[:, i].astype(jnp.float32)
        spread = spread.reshape(spread.shape[0] * spread.shape[1], spread.shape[2])
        lanes = -spread.shape[1] % LANES
        if lanes:
            spread = jnp.concatenate(
                [spread, jnp.zeros((spread.shape[0], lanes), jnp.float32)], axis=1
            )
        turned = spread.T.astype(jnp.bfloat16)
        totals = [None] * FOLD
        for q in range(FOLD):
            part = jnp.dot(
                turned[q * members : (q + 1) * members],
                table_ref[q],
                preferred_element_type=jnp.float32,
            )
            real, imag = part[:, :LANES], part[:, LANES:]
            for h in range(FOLD):
                turn = 2.0 * math.pi * (q * h % FOLD) / FOLD
                term = math.cos(turn) * real - math.sin(turn) * imag
                totals[h] = term if q == 0 else totals[h] + term
        for h in range(FOLD):
            out_ref[:, i, h * LANES : (h + 1) * LANES] = jnp.tanh(totals[h])


def coarse_kernel(
    part_modes, decay_ref, amp_ref, state_ref, noise_ref, basis_ref, next_ref, mixed_ref, fine_ref, medium_ref
):
    held, parts, modes, slots = state_ref.shape
    for scale, rate_ref in ((0, fine_ref), (1, medium_ref)):
        rate_ref[0:1] = jnp.full((1, rate_ref.shape[1]), decay_ref[scale], jnp.float32)
        rate_ref[1:2] = jnp.full((1, rate_ref.shape[1]), amp_ref[scale], jnp.float32)
    mode_ids = lax.broadcasted_iota(jnp.int32, (modes, slots), 0)
    degree_ids = lax.broadcasted_iota(jnp.int32, (modes, slots), 1)
    inside = mode_ids + degree_ids < slots
    planes = []
    for e in range(held):
        for c in range(parts):
            new = decay_ref[2] * state_ref[e, c] + amp_ref[2] * noise_ref[e, c].astype(jnp.float32)
            new = jnp.where(inside, new, 0.0)
            next_ref[e, c] = new
            planes.append(new)
    for r in range(basis_ref.shape[0]):
        planes.append(basis_ref[r].astype(jnp.float32))
    empty = jnp.zeros((part_modes, slots), jnp.float32)
    for d in range(mixed_ref.shape[0]):
        pieces = []
        for plane in planes:
            piece = plane[d * part_modes : min((d + 1) * part_modes, modes)]
            missing = part_modes - piece.shape[0]
            if missing == part_modes:
                piece = empty
            elif missing:
                piece = jnp.concatenate([piece, empty[:missing]], axis=0)
            pieces.append(piece)
        mixed_ref[d] = jnp.concatenate(pieces, axis=0).astype(jnp.bfloat16)


def body(
    fine_state,
    fine_noise,
    medium_state,
    medium_noise,
    coarse_state,
    coarse_noise,
    decay,
    amplitude,
    fine_basis,
    medium_basis,
    coarse_basis,
):
    devices = lax.axis_size("scale") * lax.axis_size("lat")
    lat = lax.axis_size("lat")
    held, _, modes, slots = coarse_state.shape
    own = coarse_basis.shape[0]
    part_modes = -(-modes // devices)
    vmem = pl.BlockSpec(memory_space=pltpu.VMEM)
    smem = pl.BlockSpec(memory_space=pltpu.SMEM)
    coarse_next, mixed, fine_rates, medium_rates = pl.pallas_call(
        functools.partial(coarse_kernel, part_modes),
        out_shape=(
            jax.ShapeDtypeStruct(coarse_state.shape, jnp.float32),
            jax.ShapeDtypeStruct((devices, (2 * held + own) * part_modes, slots), jnp.bfloat16),
            jax.ShapeDtypeStruct((2, fine_state.shape[3]), jnp.float32),
            jax.ShapeDtypeStruct((2, medium_state.shape[3]), jnp.float32),
        ),
        in_specs=[smem, smem, vmem, vmem, vmem],
        out_specs=(vmem,) * 4,
    )(decay, amplitude, coarse_state, coarse_noise, coarse_basis)
    mixed = lax.all_to_all(mixed, ("scale", "lat"), split_axis=0, concat_axis=0, tiled=True)
    mixed = mixed.reshape(devices, 2 * held + own, part_modes, slots)
    coarse_half = mixed[:lat, : 2 * held].reshape(lat * held, 2, part_modes, slots)
    coarse_rows = mixed[:, 2 * held :].reshape(devices * own, part_modes, slots)
    place = lax.axis_index(("scale", "lat"))
    fine_next = advance(fine_state, fine_noise, fine_rates[0], fine_rates[1], place * fine_state.shape[2])
    medium_next = advance(
        medium_state, medium_noise, medium_rates[0], medium_rates[1], place * medium_state.shape[2]
    )
    fourier = []
    for half, basis, form in (
        (fine_next.astype(jnp.bfloat16), fine_basis, "ecmk,mrk->rcme"),
        (medium_next.astype(jnp.bfloat16), medium_basis, "ecmk,mrk->rcme"),
        (coarse_half, coarse_rows, "ecmk,rmk->rcme"),
    ):
        fourier.append(
            jnp.einsum(form, half, basis, preferred_element_type=jnp.float32).astype(jnp.bfloat16)
        )
    members = coarse_half.shape[0]
    blocks = [x.shape[2] for x in fourier]
    both = jnp.concatenate([phase_blocks(x, place, devices) for x in fourier], axis=1)
    width = -(-both.shape[1] // 8) * 8
    both = jnp.pad(both, ((0, 0), (0, width - both.shape[1]), (0, 0)))
    received = received_rows(blocks, devices, width)
    table = pl.pallas_call(
        table_kernel,
        out_shape=jax.ShapeDtypeStruct((FOLD, devices * width, 2 * LANES), jnp.bfloat16),
        in_specs=[vmem],
        out_specs=vmem,
        cost_estimate=pl.CostEstimate(
            flops=30 * FOLD * devices * width * LANES,
            bytes_accessed=8 * FOLD * devices * width * LANES,
            transcendentals=4 * devices * width * LANES,
        ),
    )(jnp.asarray(received))
    got = lax.all_to_all(both, ("scale", "lat"), split_axis=0, concat_axis=0, tiled=True)
    got = got.reshape(devices, own, width, FOLD * members)
    pattern = pl.pallas_call(
        functools.partial(longitude_kernel, members),
        out_shape=jax.ShapeDtypeStruct((members, own, NLON), jnp.float32),
        in_specs=[vmem, vmem],
        out_specs=vmem,
    )(got, table)
    return (fine_next, medium_next, coarse_next, pattern)


def solution(mesh):
    return jax.shard_map(
        body,
        mesh=mesh,
        in_specs=(
            P(None, None, ("scale", "lat"), None),
            P(None, None, ("scale", "lat"), None),
            P(None, None, ("scale", "lat"), None),
            P(None, None, ("scale", "lat"), None),
            P("lat", None, None, None),
            P("lat", None, None, None),
            P(),
            P(),
            P(("scale", "lat"), None, None),
            P(("scale", "lat"), None, None),
            P(("scale", "lat"), None, None),
        ),
        out_specs=(
            P(None, None, ("scale", "lat"), None),
            P(None, None, ("scale", "lat"), None),
            P("lat", None, None, None),
            P(None, ("scale", "lat"), None),
        ),
        check_vma=False,
    )
```
